32 devices in a mesh: lat: 16 (over z, x, core), tm: 2 (over y).
Axes of the slice: x: 2, y: 2, z: 4, core: 2. Of those that a mesh axis runs over, the one named last changes fastest.
Arguments:
- fields: bfloat16 [512, 64, 1024], P('lat', 'tm'), may hold values from -16 to 16
Outputs:
- covariance: float32 [64, 64], P('tm')
The draws below stay inside these ranges and needn't reach their ends.
All inputs are finite; a program needn't handle non-finite values.
Results may differ from the reference program's by a relative error of at most 0.0003.
Values may be sent and summed in bfloat16 or wider, within the bound.
No kernel may reach another device: no remote copies, remote signals or barrier semaphores. Data moves between devices by JAX's collectives and lax.ppermute only.
A program may use at most 64 MiB of HBM per device.

```python
import math
import jax
import jax.numpy as jnp
from jax import lax

NLON = 1024
NLAT = 512
TRUNC = 341
MSLOT = 384
DSLOT = 384
MONTHS = 64


def draw_fields(key, part):
    patterns_count = 8
    half_lon = NLON // 2
    waves = jnp.arange(half_lon).astype(jnp.int32)
    longitude = jnp.arange(NLON).astype(jnp.int32)
    phase = 2.0 * math.pi * (waves[:, None] * longitude[None, :] % NLON).astype(jnp.float32) / NLON
    redness = 1.0 / (1.0 + waves.astype(jnp.float32) / (NLON / 2.0))
    cos_amps = jax.random.normal(jax.random.fold_in(key, 1), (patterns_count * NLAT, half_lon), jnp.float32) * redness
    sin_amps = jax.random.normal(jax.random.fold_in(key, 2), (patterns_count * NLAT, half_lon), jnp.float32) * redness
    patterns = jnp.dot(cos_amps, jnp.cos(phase)) + jnp.dot(sin_amps, jnp.sin(phase))
    patterns = patterns / jnp.sqrt(jnp.mean(patterns * patterns) + 1e-06)
    patterns = patterns.reshape(patterns_count, NLAT, NLON)
    month_amps = jax.random.normal(jax.random.fold_in(key, 3), (MONTHS, patterns_count), jnp.float32) / math.sqrt(patterns_count)
    month_scale = 1.0 + 2.0 * jnp.arange(MONTHS).astype(jnp.float32) / max(MONTHS - 1, 1)
    shared = jnp.einsum('tk,kjl->jtl', month_amps, patterns)
    noise = 0.5 * jax.random.normal(jax.random.fold_in(key, 4), (NLAT, MONTHS, NLON), jnp.float32)
    values = month_scale[None, :, None] * (shared + noise)
    return jnp.clip(values, -16.0, 16.0).astype(jnp.bfloat16)


def setup_inputs(seed: int = 0) -> dict:
    key_of = jax.random.split(jax.random.key(seed), 2)
    fields = draw_fields(jax.random.fold_in(key_of[1], 71), 0)
    return dict(fields=fields)


def start_value(order, sine_lat):
    log_start = 0.5 * (math.log(0.5) + lax.lgamma(order + 1.5) - (0.5 * math.log(math.pi) - math.log(2.0)) - lax.lgamma(order + 1.0)) + order * jnp.log(sine_lat)
    taper = jnp.clip((log_start + 70.0) / 10.0, 0.0, 1.0)
    return jnp.exp(jnp.maximum(log_start, -80.0)) * taper

def step_factors(order, degree):
    top = jnp.sqrt((4.0 * degree * degree - 1.0) / (degree * degree - order * order))
    below = degree - 1.0
    back = jnp.sqrt(jnp.maximum(below * below - order * order, 0.0) / jnp.abs(4.0 * below * below - 1.0))
    return (top, top * back)

def legendre_column(order, cosine_lat, sine_lat):
    first = start_value(order, sine_lat)

    def advance(carry, offset):
        current, previous = carry
        top, mixed = step_factors(order, order + offset)
        following = top * cosine_lat * current - mixed * previous
        return ((following, current), following)
    offsets = jnp.arange(1, DSLOT).astype(jnp.float32)
    _, later = lax.scan(advance, (first, jnp.zeros_like(first)), offsets)
    return jnp.concatenate([first[None, :], later], axis=0)

def weighted_basis(order, cosine_lat, sine_lat, weight):
    values = legendre_column(order, cosine_lat, sine_lat)
    offsets = jnp.arange(DSLOT).astype(jnp.float32)
    keep = (order + offsets <= TRUNC).astype(jnp.float32)
    factor = jnp.where(order > 0, math.sqrt(2.0), 1.0)
    table = values * keep[:, None] * weight[None, :] * factor
    return table.T.astype(jnp.bfloat16)

def reference(fields):
    longitude = jnp.arange(NLON).astype(jnp.int32)
    waves = jnp.arange(MSLOT).astype(jnp.int32)
    phase = 2.0 * math.pi * (longitude[:, None] * waves[None, :] % NLON).astype(jnp.float32) / NLON
    keep = (waves <= TRUNC).astype(jnp.float32)
    table = jnp.stack([jnp.cos(phase), -jnp.sin(phase)], axis=-1) * keep[None, :, None] / math.sqrt(NLON)
    table = table.reshape(NLON, 2 * MSLOT).astype(jnp.bfloat16)

    def per_row(row_fields):
        return jnp.dot(row_fields, table, preferred_element_type=jnp.float32).astype(jnp.bfloat16)
    fourier = lax.map(per_row, fields)
    fourier = fourier.reshape(NLAT, MONTHS, MSLOT, 2).transpose(2, 0, 1, 3)
    theta = math.pi * (jnp.arange(NLAT).astype(jnp.float32) + 0.5) / NLAT
    cosine_lat = jnp.cos(theta)
    sine_lat = jnp.sin(theta)
    weight = math.pi * sine_lat / NLAT

    def accumulate(gram, inputs):
        order_index, block = inputs
        order = order_index.astype(jnp.float32)
        basis = weighted_basis(order, cosine_lat, sine_lat, weight)
        coefficients = jnp.dot(block.reshape(NLAT, MONTHS * 2).T, basis, preferred_element_type=jnp.float32)
        coefficients = coefficients.astype(jnp.bfloat16).reshape(MONTHS, 2 * DSLOT)
        gram = gram + jnp.dot(coefficients, coefficients.T, preferred_element_type=jnp.float32)
        return (gram, None)
    gram, _ = lax.scan(accumulate, jnp.zeros((MONTHS, MONTHS), jnp.float32), (jnp.arange(MSLOT).astype(jnp.int32), fourier))
    trace = jnp.sum(jnp.diagonal(gram))
    return MONTHS * gram / (trace + 1e-06)
```

```python
import math

import numpy as np
import jax
import jax.numpy as jnp
from jax import lax
from jax.experimental import pallas as pl
from jax.experimental.pallas import tpu as pltpu
from jax.sharding import PartitionSpec as P

TRUNC = 341
LANES = 128
SUB = 8
STEPS = 32
SCALE = 2.0**16


def transform_table(lon_count, device_total, slot_total):
    order = np.arange(slot_total)[None, :] * device_total + np.arange(device_total)[:, None]
    order = order.reshape(-1, 1)
    phase = 2.0 * np.pi * (order * np.arange(lon_count)[None, :] % lon_count) / lon_count
    active = (order <= TRUNC) / np.sqrt(lon_count)
    table = np.stack([np.cos(phase) * active, -np.sin(phase) * active], axis=1)
    return table.reshape(-1, lon_count).astype(np.float32).astype(jnp.bfloat16)


def transform_kernel(table_ref, fields_ref, out_ref, scratch_ref):
    step = pl.program_id(0)
    groups = out_ref.shape[1]
    column_total, lon_count = table_ref.shape
    block = fields_ref[...].reshape(-1, lon_count)
    values = lax.dot_general(
        table_ref[...], block, (((1,), (1,)), ((), ())), preferred_element_type=jnp.float32
    )
    for part in range(values.shape[1] // LANES):
        group = step * (values.shape[1] // LANES) + part
        scratch_ref[pl.ds(group, column_total, stride=groups), :] = values[
            :, part * LANES : (part + 1) * LANES
        ]

    @pl.when(step == pl.num_programs(0) - 1)
    def _():
        out_ref[...] = scratch_ref[...].reshape(out_ref.shape).astype(out_ref.dtype)


def longitude_transform(fields, table, groups):
    row_count, month_count, lon_count = fields.shape
    column_total = table.shape[0]
    rows_step = 2 * LANES // month_count
    return pl.pallas_call(
        transform_kernel,
        grid=(row_count // rows_step,),
        in_specs=[
            pl.BlockSpec((column_total, lon_count), lambda g: (0, 0)),
            pl.BlockSpec((rows_step, month_count, lon_count), lambda g: (g, 0, 0)),
        ],
        out_specs=pl.BlockSpec((column_total, groups, LANES), lambda g: (0, 0, 0)),
        out_shape=jax.ShapeDtypeStruct((column_total, groups, LANES), jnp.bfloat16),
        scratch_shapes=[pltpu.VMEM((column_total * groups, LANES), jnp.float32)],
        name="transform",
    )(table, fields)


def basis_kernel(order_ref, cosine_ref, start_ref, out_ref, scratch_ref, *, depths, offsets):
    cosine = jnp.broadcast_to(cosine_ref[...], (SUB, cosine_ref.shape[1]))
    for base in range(0, len(depths), SUB):
        order = order_ref[base : base + SUB, :]
        lane = lax.broadcasted_iota(jnp.int32, order.shape, 1).astype(jnp.float32)
        first = start_ref[base : base + SUB, :]
        columns = scratch_ref.shape[0]
        for column in range(columns):
            scratch_ref[column, 0:SUB, :] = first[:, column * LANES : (column + 1) * LANES]

        def block(index, carry, order=order, lane=lane, columns=columns):
            current, previous = carry
            degree = order + (lane + 1.0) + (index * STEPS).astype(jnp.float32)
            top = jnp.sqrt((4.0 * degree * degree - 1.0) / (degree * degree - order * order))
            below = degree - 1.0
            back = jnp.sqrt(
                jnp.maximum(below * below - order * order, 0.0)
                / jnp.abs(4.0 * below * below - 1.0)
            )
            inside = degree <= TRUNC
            mixed = jnp.where(inside, top * back, 0.0)
            top = jnp.where(inside, top, 0.0)
            for step in range(STEPS):
                top_step = top[:, step : step + 1] * cosine
                following = top_step * current - mixed[:, step : step + 1] * previous
                row = pl.multiple_of((index * STEPS + (step + 1)) * SUB, SUB)
                for column in range(columns):
                    scratch_ref[column, pl.ds(row, SUB), :] = following[
                        :, column * LANES : (column + 1) * LANES
                    ]
                current, previous = following, current
            return current, previous

        depth_most = depths[base]
        lax.fori_loop(0, pl.cdiv(depth_most - 1, STEPS), block, (first, jnp.zeros_like(first)))
        for slot in range(base, min(base + SUB, len(depths))):
            depth = depths[slot]
            for column in range(columns):
                rows = scratch_ref[column, pl.ds(slot - base, depth, stride=SUB), :]
                out_ref[
                    offsets[slot] : offsets[slot] + depth, column * LANES : (column + 1) * LANES
                ] = rows.astype(out_ref.dtype)


def basis_blocks(order, cosine, start, depths, offsets):
    lat_total = cosine.shape[1]
    steps_most = pl.cdiv(max(depths) - 1, STEPS) * STEPS + 1
    return pl.pallas_call(
        lambda *refs: basis_kernel(*refs, depths=depths, offsets=offsets),
        out_shape=jax.ShapeDtypeStruct((sum(depths), lat_total), jnp.bfloat16),
        scratch_shapes=[pltpu.VMEM((lat_total // LANES, steps_most * SUB, LANES), jnp.float32)],
        name="basis",
    )(order, cosine, start)


def exchange_blocks(pieces):
    count = len(pieces)
    width = LANES // count
    block = lax.broadcasted_iota(jnp.int32, pieces[0].shape, 1) // width
    distance = count // 2
    while distance >= 1:
        low = (block // distance) % 2 == 0
        shift = distance * width
        following = list(pieces)
        for index in range(count):
            if (index // distance) % 2 == 0:
                first, second = pieces[index], pieces[index + distance]
                following[index] = jnp.where(low, first, pltpu.roll(second, shift, 1))
                following[index + distance] = jnp.where(
                    low, pltpu.roll(first, LANES - shift, 1), second
                )
        pieces = following
        distance //= 2
    return pieces


def gram_kernel(moved_ref, basis_ref, out_ref, *, depths, offsets, row_low):
    lat_devices, tm_devices, _, _, groups, _ = moved_ref.shape
    total = None
    for slot, depth in enumerate(depths):
        pieces = [
            moved_ref[:, tm, slot, part].astype(jnp.float32).reshape(lat_devices * groups, LANES)
            for part in range(2)
            for tm in range(tm_devices)
        ]
        tiles = []
        for begin in range(0, len(pieces), row_low):
            tiles.append(exchange_blocks(pieces[begin : begin + row_low]))
        fourier = jnp.concatenate(
            [
                jnp.concatenate([tile[row] for tile in tiles], axis=1)
                for row in range(row_low)
            ],
            axis=0,
        ).astype(jnp.bfloat16)
        basis = basis_ref[offsets[slot] : offsets[slot] + depth, :]
        coefficients = jnp.dot(basis, fourier, preferred_element_type=jnp.float32)
        coefficients = coefficients.astype(jnp.bfloat16)
        gram = lax.dot_general(
            coefficients,
            coefficients,
            (((0,), (0,)), ((), ())),
            preferred_element_type=jnp.float32,
        )
        total = gram if total is None else total + gram
    months = total.shape[0] // 2
    total = total * (1.0 / (SCALE * SCALE))
    if months * 2 == LANES:
        half = months // 2
        lane = lax.broadcasted_iota(jnp.int32, (half, LANES), 1)
        low = total[0:half] + pltpu.roll(total[months : months + half], months, 1)
        high = pltpu.roll(total[half:months], months, 1) + total[months + half :]
        out_ref[...] = jnp.where(lane < months, low, high)
    else:
        out_ref[...] = total[:months, :months] + total[months:, months:]


def gram_terms(moved, basis, depths, offsets, row_low):
    months = moved.shape[1] * (LANES // row_low)
    shape = (months // 2, LANES) if 2 * months == LANES else (months, months)
    return pl.pallas_call(
        lambda *refs: gram_kernel(*refs, depths=depths, offsets=offsets, row_low=row_low),
        out_shape=jax.ShapeDtypeStruct(shape, jnp.float32),
        name="gram",
    )(moved, basis)


def finish_kernel(parts_ref, out_ref):
    month_total = out_ref.shape[1]
    half = month_total // 2
    total = jnp.sum(parts_ref[...], axis=0)
    row = lax.broadcasted_iota(jnp.int32, total.shape, 0)
    lane = lax.broadcasted_iota(jnp.int32, total.shape, 1)
    diagonal = (lane == row) | (lane == row + (month_total + half))
    trace = jnp.sum(jnp.where(diagonal, total, 0.0))
    total = month_total * total / (trace + 1e-06)
    upper = lax.axis_index("tm") * jnp.ones_like(lane) == 1
    total = jnp.where(upper, pltpu.roll(total, month_total, 1), total)
    out_ref[...] = total[:, :month_total]


def local(fields):
    row_count, month_count, lon_count = fields.shape
    lat_devices = lax.axis_size("lat")
    tm_devices = lax.axis_size("tm")
    device_total = lat_devices * tm_devices
    device = lax.axis_index("lat") * tm_devices + lax.axis_index("tm")
    lat_count = row_count * lat_devices
    months = month_count * tm_devices
    slots = -(-(TRUNC + 1) // device_total)
    row_low = LANES // month_count
    groups = row_count // row_low
    depths = [-(-(TRUNC + 1 - slot * device_total) // 16) * 16 for slot in range(slots)]
    offsets = [sum(depths[:slot]) for slot in range(slots)]

    table = jnp.asarray(transform_table(lon_count, device_total, slots))
    fourier = longitude_transform(fields, table, groups)
    fourier = fourier.reshape(device_total, slots * 2, groups, LANES)
    moved = lax.all_to_all(fourier, ("lat", "tm"), split_axis=0, concat_axis=0, tiled=True)
    moved = moved.reshape(lat_devices, tm_devices, slots, 2, groups, LANES)

    latitude = np.arange(lat_count).reshape(lat_devices, groups, row_low)
    latitude = jnp.asarray(latitude.transpose(2, 0, 1).reshape(1, -1))
    theta = math.pi * (latitude.astype(jnp.float32) + 0.5) / lat_count
    cosine_lat = jnp.cos(theta)
    sine_lat = jnp.sin(theta)
    weight = math.pi * sine_lat / lat_count
    padded = -(-slots // SUB) * SUB
    order = (jnp.arange(padded) * device_total + device).astype(jnp.float32)[:, None]
    log_start = 0.5 * (
        math.log(0.5)
        + lax.lgamma(order + 1.5)
        - (0.5 * math.log(math.pi) - math.log(2.0))
        - lax.lgamma(order + 1.0)
    ) + order * jnp.log(sine_lat)
    taper = jnp.clip((log_start + 70.0) / 10.0, 0.0, 1.0)
    factor = jnp.where(order > 0, math.sqrt(2.0), 1.0) * (order <= TRUNC) * SCALE
    start = jnp.exp(jnp.maximum(log_start, -80.0)) * taper * weight * factor
    basis = basis_blocks(
        jnp.broadcast_to(order, (padded, LANES)), cosine_lat, start, depths, offsets
    )

    gram = gram_terms(moved, basis, depths, offsets, row_low)
    if 2 * months == LANES and tm_devices == 2:
        parts = lax.all_gather(gram, ("lat", "tm"), axis=0, tiled=False)
        return pl.pallas_call(
            finish_kernel,
            out_shape=jax.ShapeDtypeStruct((month_count, months), jnp.float32),
            name="finish",
        )(parts)
    gram = lax.psum(gram, ("lat", "tm")).reshape(-1)
    if 2 * months == LANES:
        gram = gram.reshape(months // 2, 2, months).transpose(1, 0, 2)
    gram = gram.reshape(months, months)
    trace = jnp.sum(jnp.diagonal(gram))
    own = lax.dynamic_slice_in_dim(gram, lax.axis_index("tm") * month_count, month_count, 0)
    return months * own / (trace + 1e-06)


def solution(mesh):
    placed = (P("lat", "tm", None),)
    return jax.shard_map(
        local, mesh=mesh, in_specs=placed, out_specs=P("tm", None), check_vma=False
    )
```

```python
import math

import numpy as np
import jax
import jax.numpy as jnp
from jax import lax
from jax.experimental import pallas as pl
from jax.experimental.pallas import tpu as pltpu
from jax.sharding import PartitionSpec as P

TRUNC = 341
LANES = 128
SUB = 8
STEPS = 32
SCALE = 2.0**16


def transform_table(lon_count, device_total, slot_total):
    order = np.arange(slot_total)[None, :] * device_total + np.arange(device_total)[:, None]
    order = order.reshape(-1, 1)
    phase = 2.0 * np.pi * (order * np.arange(lon_count)[None, :] % lon_count) / lon_count
    active = (order <= TRUNC) / np.sqrt(lon_count)
    table = np.stack([np.cos(phase) * active, -np.sin(phase) * active], axis=1)
    return table.reshape(-1, lon_count).astype(np.float32).astype(jnp.bfloat16)


def transform_kernel(table_ref, fields_ref, out_ref, scratch_ref):
    step = pl.program_id(0)
    groups = out_ref.shape[1]
    column_total, lon_count = table_ref.shape
    block = fields_ref[...].reshape(-1, lon_count)
    values = lax.dot_general(
        table_ref[...], block, (((1,), (1,)), ((), ())), preferred_element_type=jnp.float32
    )
    for part in range(values.shape[1] // LANES):
        group = step * (values.shape[1] // LANES) + part
        scratch_ref[pl.ds(group, column_total, stride=groups), :] = values[
            :, part * LANES : (part + 1) * LANES
        ]

    @pl.when(step == pl.num_programs(0) - 1)
    def _():
        out_ref[...] = scratch_ref[...].reshape(out_ref.shape).astype(out_ref.dtype)


def longitude_transform(fields, table, groups):
    row_count, month_count, lon_count = fields.shape
    column_total = table.shape[0]
    rows_step = 2 * LANES // month_count
    return pl.pallas_call(
        transform_kernel,
        grid=(row_count // rows_step,),
        in_specs=[
            pl.BlockSpec((column_total, lon_count), lambda g: (0, 0)),
            pl.BlockSpec((rows_step, month_count, lon_count), lambda g: (g, 0, 0)),
        ],
        out_specs=pl.BlockSpec((column_total, groups, LANES), lambda g: (0, 0, 0)),
        out_shape=jax.ShapeDtypeStruct((column_total, groups, LANES), jnp.bfloat16),
        scratch_shapes=[pltpu.VMEM((column_total * groups, LANES), jnp.float32)],
        name="transform",
    )(table, fields)


def basis_kernel(order_ref, cosine_ref, start_ref, out_ref, scratch_ref, *, depths, offsets):
    cosine = jnp.broadcast_to(cosine_ref[...], (SUB, cosine_ref.shape[1]))
    for base in range(0, len(depths), SUB):
        order = order_ref[base : base + SUB, :]
        lane = lax.broadcasted_iota(jnp.int32, order.shape, 1).astype(jnp.float32)
        first = start_ref[base : base + SUB, :]
        columns = scratch_ref.shape[0]
        for column in range(columns):
            scratch_ref[column, 0:SUB, :] = first[:, column * LANES : (column + 1) * LANES]

        def block(index, carry, order=order, lane=lane, columns=columns):
            current, previous = carry
            degree = order + (lane + 1.0) + (index * STEPS).astype(jnp.float32)
            top = jnp.sqrt((4.0 * degree * degree - 1.0) / (degree * degree - order * order))
            below = degree - 1.0
            back = jnp.sqrt(
                jnp.maximum(below * below - order * order, 0.0)
                / jnp.abs(4.0 * below * below - 1.0)
            )
            inside = degree <= TRUNC
            mixed = jnp.where(inside, top * back, 0.0)
            top = jnp.where(inside, top, 0.0)
            for step in range(STEPS):
                top_step = top[:, step : step + 1] * cosine
                following = top_step * current - mixed[:, step : step + 1] * previous
                row = pl.multiple_of((index * STEPS + (step + 1)) * SUB, SUB)
                for column in range(columns):
                    scratch_ref[column, pl.ds(row, SUB), :] = following[
                        :, column * LANES : (column + 1) * LANES
                    ]
                current, previous = following, current
            return current, previous

        depth_most = depths[base]
        lax.fori_loop(0, pl.cdiv(depth_most - 1, STEPS), block, (first, jnp.zeros_like(first)))
        for slot in range(base, min(base + SUB, len(depths))):
            depth = depths[slot]
            for column in range(columns):
                rows = scratch_ref[column, pl.ds(slot - base, depth, stride=SUB), :]
                out_ref[
                    offsets[slot] : offsets[slot] + depth, column * LANES : (column + 1) * LANES
                ] = rows.astype(out_ref.dtype)


def basis_blocks(order, cosine, start, depths, offsets):
    lat_total = cosine.shape[1]
    steps_most = pl.cdiv(max(depths) - 1, STEPS) * STEPS + 1
    return pl.pallas_call(
        lambda *refs: basis_kernel(*refs, depths=depths, offsets=offsets),
        out_shape=jax.ShapeDtypeStruct((sum(depths), lat_total), jnp.bfloat16),
        scratch_shapes=[pltpu.VMEM((lat_total // LANES, steps_most * SUB, LANES), jnp.float32)],
        name="basis",
    )(order, cosine, start)


def exchange_blocks(pieces):
    count = len(pieces)
    width = LANES // count
    block = lax.broadcasted_iota(jnp.int32, pieces[0].shape, 1) // width
    distance = count // 2
    while distance >= 1:
        low = (block // distance) % 2 == 0
        shift = distance * width
        following = list(pieces)
        for index in range(count):
            if (index // distance) % 2 == 0:
                first, second = pieces[index], pieces[index + distance]
                following[index] = jnp.where(low, first, pltpu.roll(second, shift, 1))
                following[index + distance] = jnp.where(
                    low, pltpu.roll(first, LANES - shift, 1), second
                )
        pieces = following
        distance //= 2
    return pieces


def gram_kernel(moved_ref, basis_ref, out_ref, *, depths, offsets, row_low):
    lat_devices, tm_devices, _, _, groups, _ = moved_ref.shape
    total = None
    for slot, depth in enumerate(depths):
        pieces = [
            moved_ref[:, tm, slot, part].astype(jnp.float32).reshape(lat_devices * groups, LANES)
            for part in range(2)
            for tm in range(tm_devices)
        ]
        tiles = []
        for begin in range(0, len(pieces), row_low):
            tiles.append(exchange_blocks(pieces[begin : begin + row_low]))
        fourier = jnp.concatenate(
            [
                jnp.concatenate([tile[row] for tile in tiles], axis=1)
                for row in range(row_low)
            ],
            axis=0,
        ).astype(jnp.bfloat16)
        basis = basis_ref[offsets[slot] : offsets[slot] + depth, :]
        coefficients = jnp.dot(basis, fourier, preferred_element_type=jnp.float32)
        coefficients = coefficients.astype(jnp.bfloat16)
        gram = lax.dot_general(
            coefficients,
            coefficients,
            (((0,), (0,)), ((), ())),
            preferred_element_type=jnp.float32,
        )
        total = gram if total is None else total + gram
    months = total.shape[0] // 2
    total = total * (1.0 / (SCALE * SCALE))
    if len(out_ref.shape) == 2:
        out_ref[...] = total[:months, :months] + total[months:, months:]
        return
    half = months // 2
    quarter = half // 2
    lane = lax.broadcasted_iota(jnp.int32, (half, LANES), 1)
    row = lax.broadcasted_iota(jnp.int32, (half, LANES), 0)
    low = total[0:half] + pltpu.roll(total[months : months + half], months, 1)
    high = pltpu.roll(total[half:months], months, 1) + total[months + half :]
    packed = jnp.where(lane < months, low, high)
    trace = jnp.sum(jnp.where((lane == row) | (lane == row + months + half), packed, 0.0))
    lane = lane[:quarter]
    row = row[:quarter]
    swapped = pltpu.roll(packed, months, 1)
    halves = (
        jnp.where(lane < months, packed[:quarter], swapped[quarter:]),
        jnp.where(lane < months, swapped[:quarter], packed[quarter:]),
    )
    for index, value in enumerate(halves):
        value = jnp.where((row == 1) & (lane == index * half), trace, value)
        for device in range(index, out_ref.shape[0], 2):
            out_ref[device] = value


def gram_terms(moved, basis, depths, offsets, row_low, spread):
    months = moved.shape[1] * (LANES // row_low)
    shape = (spread, months // 4, LANES) if spread else (months, months)
    return pl.pallas_call(
        lambda *refs: gram_kernel(*refs, depths=depths, offsets=offsets, row_low=row_low),
        out_shape=jax.ShapeDtypeStruct(shape, jnp.float32),
        name="gram",
    )(moved, basis)


def finish_kernel(parts_ref, out_ref):
    half, month_total = out_ref.shape
    total = jnp.sum(parts_ref[...], axis=0)
    row = lax.broadcasted_iota(jnp.int32, total.shape, 0)
    lane = lax.broadcasted_iota(jnp.int32, total.shape, 1)
    corner = lane - lax.axis_index("tm") * half
    slot = (row == 1) & (corner == 0)
    trace = jnp.sum(jnp.where(slot, total, 0.0))
    mirror = jnp.sum(jnp.where((row == 0) & (corner == 1), total, 0.0))
    total = jnp.where(slot, mirror, total)
    total = month_total * total / (trace + 1e-06)
    out_ref[: half // 2] = total[:, :month_total]
    out_ref[half // 2 :] = pltpu.roll(total, month_total, 1)[:, :month_total]


def local(fields):
    row_count, month_count, lon_count = fields.shape
    lat_devices = lax.axis_size("lat")
    tm_devices = lax.axis_size("tm")
    device_total = lat_devices * tm_devices
    device = lax.axis_index("lat") * tm_devices + lax.axis_index("tm")
    lat_count = row_count * lat_devices
    months = month_count * tm_devices
    slots = -(-(TRUNC + 1) // device_total)
    row_low = LANES // month_count
    groups = row_count // row_low
    depths = [-(-(TRUNC + 1 - slot * device_total) // 16) * 16 for slot in range(slots)]
    offsets = [sum(depths[:slot]) for slot in range(slots)]

    table = jnp.asarray(transform_table(lon_count, device_total, slots))
    fourier = longitude_transform(fields, table, groups)
    fourier = fourier.reshape(device_total, slots * 2, groups, LANES)
    moved = lax.all_to_all(fourier, ("lat", "tm"), split_axis=0, concat_axis=0, tiled=True)
    moved = moved.reshape(lat_devices, tm_devices, slots, 2, groups, LANES)

    latitude = np.arange(lat_count).reshape(lat_devices, groups, row_low)
    latitude = jnp.asarray(latitude.transpose(2, 0, 1).reshape(1, -1))
    theta = math.pi * (latitude.astype(jnp.float32) + 0.5) / lat_count
    cosine_lat = jnp.cos(theta)
    sine_lat = jnp.sin(theta)
    weight = math.pi * sine_lat / lat_count
    padded = -(-slots // SUB) * SUB
    order = (jnp.arange(padded) * device_total + device).astype(jnp.float32)[:, None]
    log_start = 0.5 * (
        math.log(0.5)
        + lax.lgamma(order + 1.5)
        - (0.5 * math.log(math.pi) - math.log(2.0))
        - lax.lgamma(order + 1.0)
    ) + order * jnp.log(sine_lat)
    taper = jnp.clip((log_start + 70.0) / 10.0, 0.0, 1.0)
    factor = jnp.where(order > 0, math.sqrt(2.0), 1.0) * (order <= TRUNC) * SCALE
    start = jnp.exp(jnp.maximum(log_start, -80.0)) * taper * weight * factor
    basis = basis_blocks(
        jnp.broadcast_to(order, (padded, LANES)), cosine_lat, start, depths, offsets
    )

    spread = device_total if 2 * months == LANES and tm_devices == 2 else 0
    gram = gram_terms(moved, basis, depths, offsets, row_low, spread)
    if spread:
        parts = lax.all_to_all(gram, ("lat", "tm"), split_axis=0, concat_axis=0, tiled=True)
        return pl.pallas_call(
            finish_kernel,
            out_shape=jax.ShapeDtypeStruct((month_count, months), jnp.float32),
            name="finish",
        )(parts)
    gram = lax.psum(gram, ("lat", "tm"))
    trace = jnp.sum(jnp.diagonal(gram))
    own = lax.dynamic_slice_in_dim(gram, lax.axis_index("tm") * month_count, month_count, 0)
    return months * own / (trace + 1e-06)


def solution(mesh):
    placed = (P("lat", "tm", None),)
    return jax.shard_map(
        local, mesh=mesh, in_specs=placed, out_specs=P("tm", None), check_vma=False
    )
```

```python
import math

import numpy as np
import jax
import jax.numpy as jnp
from jax import lax
from jax.experimental import pallas as pl
from jax.experimental.pallas import tpu as pltpu
from jax.sharding import PartitionSpec as P

TRUNC = 341
LANES = 128
SUB = 8
STEPS = 32
SCALE = 2.0**16
PARAMS = pltpu.CompilerParams(vmem_limit_bytes=32 * 2**20)


def transform_table(lon_count, device_total, slot_total):
    order = np.arange(slot_total)[None, :] * device_total + np.arange(device_total)[:, None]
    order = order.reshape(-1, 1)
    phase = 2.0 * np.pi * (order * np.arange(lon_count)[None, :] % lon_count) / lon_count
    active = (order <= TRUNC) / np.sqrt(lon_count)
    table = np.stack([np.cos(phase) * active, -np.sin(phase) * active], axis=1)
    return table.reshape(-1, lon_count).astype(np.float32).astype(jnp.bfloat16)


def transform_kernel(table_ref, fields_ref, out_ref, scratch_ref):
    step = pl.program_id(0)
    groups = out_ref.shape[1]
    column_total, lon_count = table_ref.shape
    block = fields_ref[...].reshape(-1, lon_count)
    values = lax.dot_general(
        table_ref[...], block, (((1,), (1,)), ((), ())), preferred_element_type=jnp.float32
    )
    for part in range(values.shape[1] // LANES):
        group = step * (values.shape[1] // LANES) + part
        scratch_ref[pl.ds(group, column_total, stride=groups), :] = values[
            :, part * LANES : (part + 1) * LANES
        ]

    @pl.when(step == pl.num_programs(0) - 1)
    def _():
        out_ref[...] = scratch_ref[...].reshape(out_ref.shape).astype(out_ref.dtype)


def longitude_transform(fields, table, groups):
    row_count, month_count, lon_count = fields.shape
    column_total = table.shape[0]
    rows_step = 2 * LANES // month_count
    return pl.pallas_call(
        transform_kernel,
        grid=(row_count // rows_step,),
        in_specs=[
            pl.BlockSpec((column_total, lon_count), lambda g: (0, 0)),
            pl.BlockSpec((rows_step, month_count, lon_count), lambda g: (g, 0, 0)),
        ],
        out_specs=pl.BlockSpec((column_total, groups, LANES), lambda g: (0, 0, 0)),
        out_shape=jax.ShapeDtypeStruct((column_total, groups, LANES), jnp.bfloat16),
        scratch_shapes=[pltpu.VMEM((column_total * groups, LANES), jnp.float32)],
        compiler_params=PARAMS,
        name="transform",
    )(table, fields)


def basis_kernel(order_ref, cosine_ref, start_ref, out_ref, scratch_ref, *, depths, offsets):
    cosine = jnp.broadcast_to(cosine_ref[...], (SUB, cosine_ref.shape[1]))
    for base in range(0, len(depths), SUB):
        order = order_ref[base : base + SUB, :]
        lane = lax.broadcasted_iota(jnp.int32, order.shape, 1).astype(jnp.float32)
        first = start_ref[base : base + SUB, :]
        columns = scratch_ref.shape[0]
        for column in range(columns):
            scratch_ref[column, 0:SUB, :] = first[:, column * LANES : (column + 1) * LANES]

        def block(index, carry, order=order, lane=lane, columns=columns):
            current, previous = carry
            degree = order + (lane + 1.0) + (index * STEPS).astype(jnp.float32)
            top = jnp.sqrt((4.0 * degree * degree - 1.0) / (degree * degree - order * order))
            below = degree - 1.0
            back = jnp.sqrt(
                jnp.maximum(below * below - order * order, 0.0)
                / jnp.abs(4.0 * below * below - 1.0)
            )
            inside = degree <= TRUNC
            mixed = jnp.where(inside, top * back, 0.0)
            top = jnp.where(inside, top, 0.0)
            for step in range(STEPS):
                top_step = top[:, step : step + 1] * cosine
                following = top_step * current - mixed[:, step : step + 1] * previous
                row = pl.multiple_of((index * STEPS + (step + 1)) * SUB, SUB)
                for column in range(columns):
                    scratch_ref[column, pl.ds(row, SUB), :] = following[
                        :, column * LANES : (column + 1) * LANES
                    ]
                current, previous = following, current
            return current, previous

        depth_most = depths[base]
        lax.fori_loop(0, pl.cdiv(depth_most - 1, STEPS), block, (first, jnp.zeros_like(first)))
        for slot in range(base, min(base + SUB, len(depths))):
            depth = depths[slot]
            for column in range(columns):
                rows = scratch_ref[column, pl.ds(slot - base, depth, stride=SUB), :]
                out_ref[
                    offsets[slot] : offsets[slot] + depth, column * LANES : (column + 1) * LANES
                ] = rows.astype(out_ref.dtype)


def basis_blocks(order, cosine, start, depths, offsets):
    lat_total = cosine.shape[1]
    steps_most = pl.cdiv(max(depths) - 1, STEPS) * STEPS + 1
    return pl.pallas_call(
        lambda *refs: basis_kernel(*refs, depths=depths, offsets=offsets),
        out_shape=pltpu.VMEM((sum(depths), lat_total), jnp.bfloat16),
        scratch_shapes=[pltpu.VMEM((lat_total // LANES, steps_most * SUB, LANES), jnp.float32)],
        out_specs=pl.BlockSpec(memory_space=pltpu.VMEM),
        compiler_params=PARAMS,
        name="basis",
    )(order, cosine, start)


def exchange_blocks(pieces):
    count = len(pieces)
    width = LANES // count
    block = lax.broadcasted_iota(jnp.int32, pieces[0].shape, 1) // width
    distance = count // 2
    while distance >= 1:
        low = (block // distance) % 2 == 0
        shift = distance * width
        following = list(pieces)
        for index in range(count):
            if (index // distance) % 2 == 0:
                first, second = pieces[index], pieces[index + distance]
                following[index] = jnp.where(low, first, pltpu.roll(second, shift, 1))
                following[index + distance] = jnp.where(
                    low, pltpu.roll(first, LANES - shift, 1), second
                )
        pieces = following
        distance //= 2
    return pieces


def gram_kernel(moved_ref, basis_ref, out_ref, *, depths, offsets, row_low):
    lat_devices, tm_devices, _, _, groups, _ = moved_ref.shape
    total = None
    for slot, depth in enumerate(depths):
        pieces = [
            moved_ref[:, tm, slot, part].astype(jnp.float32).reshape(lat_devices * groups, LANES)
            for part in range(2)
            for tm in range(tm_devices)
        ]
        tiles = []
        for begin in range(0, len(pieces), row_low):
            tiles.append(exchange_blocks(pieces[begin : begin + row_low]))
        fourier = jnp.concatenate(
            [
                jnp.concatenate([tile[row] for tile in tiles], axis=1)
                for row in range(row_low)
            ],
            axis=0,
        ).astype(jnp.bfloat16)
        basis = basis_ref[offsets[slot] : offsets[slot] + depth, :]
        coefficients = jnp.dot(basis, fourier, preferred_element_type=jnp.float32)
        coefficients = coefficients.astype(jnp.bfloat16)
        gram = lax.dot_general(
            coefficients,
            coefficients,
            (((0,), (0,)), ((), ())),
            preferred_element_type=jnp.float32,
        )
        total = gram if total is None else total + gram
    months = total.shape[0] // 2
    total = total * (1.0 / (SCALE * SCALE))
    if len(out_ref.shape) == 2:
        out_ref[...] = total[:months, :months] + total[months:, months:]
        return
    half = months // 2
    quarter = half // 2
    lane = lax.broadcasted_iota(jnp.int32, (half, LANES), 1)
    row = lax.broadcasted_iota(jnp.int32, (half, LANES), 0)
    low = total[0:half] + pltpu.roll(total[months : months + half], months, 1)
    high = pltpu.roll(total[half:months], months, 1) + total[months + half :]
    packed = jnp.where(lane < months, low, high)
    trace = jnp.sum(jnp.where((lane == row) | (lane == row + months + half), packed, 0.0))
    lane = lane[:quarter]
    row = row[:quarter]
    swapped = pltpu.roll(packed, months, 1)
    halves = (
        jnp.where(lane < months, packed[:quarter], swapped[quarter:]),
        jnp.where(lane < months, swapped[:quarter], packed[quarter:]),
    )
    for index, value in enumerate(halves):
        value = jnp.where((row == 1) & (lane == index * half), trace, value)
        for device in range(index, out_ref.shape[0], 2):
            out_ref[device] = value


def gram_terms(moved, basis, depths, offsets, row_low, spread):
    months = moved.shape[1] * (LANES // row_low)
    shape = (spread, months // 4, LANES) if spread else (months, months)
    return pl.pallas_call(
        lambda *refs: gram_kernel(*refs, depths=depths, offsets=offsets, row_low=row_low),
        in_specs=[pl.BlockSpec(memory_space=pltpu.VMEM)] * 2,
        out_specs=pl.BlockSpec(memory_space=pltpu.VMEM),
        out_shape=pltpu.VMEM(shape, jnp.float32),
        compiler_params=PARAMS,
        name="gram",
    )(
        pltpu.with_memory_space_constraint(moved, pltpu.VMEM),
        pltpu.with_memory_space_constraint(basis, pltpu.VMEM),
    )


def finish_kernel(parts_ref, out_ref):
    half, month_total = out_ref.shape
    total = jnp.sum(parts_ref[...], axis=0)
    row = lax.broadcasted_iota(jnp.int32, total.shape, 0)
    lane = lax.broadcasted_iota(jnp.int32, total.shape, 1)
    corner = lane - lax.axis_index("tm") * half
    slot = (row == 1) & (corner == 0)
    trace = jnp.sum(jnp.where(slot, total, 0.0))
    mirror = jnp.sum(jnp.where((row == 0) & (corner == 1), total, 0.0))
    total = jnp.where(slot, mirror, total)
    total = month_total * total / (trace + 1e-06)
    out_ref[: half // 2] = total[:, :month_total]
    out_ref[half // 2 :] = pltpu.roll(total, month_total, 1)[:, :month_total]


def local(fields):
    row_count, month_count, lon_count = fields.shape
    lat_devices = lax.axis_size("lat")
    tm_devices = lax.axis_size("tm")
    device_total = lat_devices * tm_devices
    device = lax.axis_index("lat") * tm_devices + lax.axis_index("tm")
    lat_count = row_count * lat_devices
    months = month_count * tm_devices
    slots = -(-(TRUNC + 1) // device_total)
    row_low = LANES // month_count
    groups = row_count // row_low
    depths = [-(-(TRUNC + 1 - slot * device_total) // 16) * 16 for slot in range(slots)]
    offsets = [sum(depths[:slot]) for slot in range(slots)]

    table = jnp.asarray(transform_table(lon_count, device_total, slots))
    fourier = longitude_transform(fields, table, groups)
    fourier = fourier.reshape(device_total, slots * 2, groups, LANES)
    moved = lax.all_to_all(fourier, ("lat", "tm"), split_axis=0, concat_axis=0, tiled=True)
    moved = moved.reshape(lat_devices, tm_devices, slots, 2, groups, LANES)

    latitude = np.arange(lat_count).reshape(lat_devices, groups, row_low)
    latitude = jnp.asarray(latitude.transpose(2, 0, 1).reshape(1, -1))
    theta = math.pi * (latitude.astype(jnp.float32) + 0.5) / lat_count
    cosine_lat = jnp.cos(theta)
    sine_lat = jnp.sin(theta)
    weight = math.pi * sine_lat / lat_count
    padded = -(-slots // SUB) * SUB
    order = (jnp.arange(padded) * device_total + device).astype(jnp.float32)[:, None]
    log_start = 0.5 * (
        math.log(0.5)
        + lax.lgamma(order + 1.5)
        - (0.5 * math.log(math.pi) - math.log(2.0))
        - lax.lgamma(order + 1.0)
    ) + order * jnp.log(sine_lat)
    taper = jnp.clip((log_start + 70.0) / 10.0, 0.0, 1.0)
    factor = jnp.where(order > 0, math.sqrt(2.0), 1.0) * (order <= TRUNC) * SCALE
    start = jnp.exp(jnp.maximum(log_start, -80.0)) * taper * weight * factor
    basis = basis_blocks(
        jnp.broadcast_to(order, (padded, LANES)), cosine_lat, start, depths, offsets
    )

    spread = device_total if 2 * months == LANES and tm_devices == 2 else 0
    gram = gram_terms(moved, basis, depths, offsets, row_low, spread)
    if spread:
        parts = lax.all_to_all(gram, ("lat", "tm"), split_axis=0, concat_axis=0, tiled=True)
        return pl.pallas_call(
            finish_kernel,
            out_shape=jax.ShapeDtypeStruct((month_count, months), jnp.float32),
            compiler_params=PARAMS,
        name="finish",
        )(parts)
    gram = lax.psum(gram, ("lat", "tm"))
    trace = jnp.sum(jnp.diagonal(gram))
    own = lax.dynamic_slice_in_dim(gram, lax.axis_index("tm") * month_count, month_count, 0)
    return months * own / (trace + 1e-06)


def solution(mesh):
    placed = (P("lat", "tm", None),)
    return jax.shard_map(
        local, mesh=mesh, in_specs=placed, out_specs=P("tm", None), check_vma=False
    )
```

```python
import math

import numpy as np
import jax
import jax.numpy as jnp
from jax import lax
from jax.experimental import pallas as pl
from jax.experimental.pallas import tpu as pltpu
from jax.sharding import PartitionSpec as P

TRUNC = 341
LANES = 128
SUB = 8
STEPS = 32
SCALE = 2.0**16
PARAMS = pltpu.CompilerParams(vmem_limit_bytes=32 * 2**20)


def transform_table(lon_count, device_total, slot_total):
    order = np.arange(slot_total)[None, :] * device_total + np.arange(device_total)[:, None]
    order = order.reshape(-1, 1)
    phase = 2.0 * np.pi * (order * np.arange(lon_count)[None, :] % lon_count) / lon_count
    active = (order <= TRUNC) / np.sqrt(lon_count)
    table = np.stack([np.cos(phase) * active, -np.sin(phase) * active], axis=1)
    return table.reshape(-1, lon_count).astype(np.float32).astype(jnp.bfloat16)


def transform_kernel(table_ref, fields_ref, out_ref, scratch_ref):
    step = pl.program_id(0)
    groups = out_ref.shape[1]
    column_total, lon_count = table_ref.shape
    block = fields_ref[...].reshape(-1, lon_count)
    values = lax.dot_general(
        table_ref[...], block, (((1,), (1,)), ((), ())), preferred_element_type=jnp.float32
    )
    for part in range(values.shape[1] // LANES):
        group = step * (values.shape[1] // LANES) + part
        scratch_ref[pl.ds(group, column_total, stride=groups), :] = values[
            :, part * LANES : (part + 1) * LANES
        ]

    @pl.when(step == pl.num_programs(0) - 1)
    def _():
        out_ref[...] = scratch_ref[...].reshape(out_ref.shape).astype(out_ref.dtype)


def longitude_transform(fields, table, groups):
    row_count, month_count, lon_count = fields.shape
    column_total = table.shape[0]
    rows_step = 2 * LANES // month_count
    return pl.pallas_call(
        transform_kernel,
        grid=(row_count // rows_step,),
        in_specs=[
            pl.BlockSpec((column_total, lon_count), lambda g: (0, 0)),
            pl.BlockSpec((rows_step, month_count, lon_count), lambda g: (g, 0, 0)),
        ],
        out_specs=pl.BlockSpec((column_total, groups, LANES), lambda g: (0, 0, 0)),
        out_shape=jax.ShapeDtypeStruct((column_total, groups, LANES), jnp.bfloat16),
        scratch_shapes=[pltpu.VMEM((column_total * groups, LANES), jnp.float32)],
        compiler_params=PARAMS,
        name="transform",
    )(
        pltpu.with_memory_space_constraint(table, pltpu.HBM),
        pltpu.with_memory_space_constraint(fields, pltpu.HBM),
    )


def basis_kernel(order_ref, cosine_ref, start_ref, out_ref, scratch_ref, *, depths, offsets):
    cosine = jnp.broadcast_to(cosine_ref[...], (SUB, cosine_ref.shape[1]))
    for base in range(0, len(depths), SUB):
        order = order_ref[base : base + SUB, :]
        lane = lax.broadcasted_iota(jnp.int32, order.shape, 1).astype(jnp.float32)
        first = start_ref[base : base + SUB, :]
        columns = scratch_ref.shape[0]
        for column in range(columns):
            scratch_ref[column, 0:SUB, :] = first[:, column * LANES : (column + 1) * LANES]

        def block(index, carry, order=order, lane=lane, columns=columns):
            current, previous = carry
            degree = order + (lane + 1.0) + (index * STEPS).astype(jnp.float32)
            top = jnp.sqrt((4.0 * degree * degree - 1.0) / (degree * degree - order * order))
            below = degree - 1.0
            back = jnp.sqrt(
                jnp.maximum(below * below - order * order, 0.0)
                / jnp.abs(4.0 * below * below - 1.0)
            )
            inside = degree <= TRUNC
            mixed = jnp.where(inside, top * back, 0.0)
            top = jnp.where(inside, top, 0.0)
            for step in range(STEPS):
                top_step = top[:, step : step + 1] * cosine
                following = top_step * current - mixed[:, step : step + 1] * previous
                row = pl.multiple_of((index * STEPS + (step + 1)) * SUB, SUB)
                for column in range(columns):
                    scratch_ref[column, pl.ds(row, SUB), :] = following[
                        :, column * LANES : (column + 1) * LANES
                    ]
                current, previous = following, current
            return current, previous

        depth_most = depths[base]
        lax.fori_loop(0, pl.cdiv(depth_most - 1, STEPS), block, (first, jnp.zeros_like(first)))
        for slot in range(base, min(base + SUB, len(depths))):
            depth = depths[slot]
            for column in range(columns):
                rows = scratch_ref[column, pl.ds(slot - base, depth, stride=SUB), :]
                out_ref[
                    offsets[slot] : offsets[slot] + depth, column * LANES : (column + 1) * LANES
                ] = rows.astype(out_ref.dtype)


def basis_blocks(order, cosine, start, depths, offsets):
    lat_total = cosine.shape[1]
    steps_most = pl.cdiv(max(depths) - 1, STEPS) * STEPS + 1
    return pl.pallas_call(
        lambda *refs: basis_kernel(*refs, depths=depths, offsets=offsets),
        out_shape=pltpu.VMEM((sum(depths), lat_total), jnp.bfloat16),
        scratch_shapes=[pltpu.VMEM((lat_total // LANES, steps_most * SUB, LANES), jnp.float32)],
        out_specs=pl.BlockSpec(memory_space=pltpu.VMEM),
        compiler_params=PARAMS,
        name="basis",
    )(order, cosine, start)


def exchange_blocks(pieces):
    count = len(pieces)
    width = LANES // count
    block = lax.broadcasted_iota(jnp.int32, pieces[0].shape, 1) // width
    distance = count // 2
    while distance >= 1:
        low = (block // distance) % 2 == 0
        shift = distance * width
        following = list(pieces)
        for index in range(count):
            if (index // distance) % 2 == 0:
                first, second = pieces[index], pieces[index + distance]
                following[index] = jnp.where(low, first, pltpu.roll(second, shift, 1))
                following[index + distance] = jnp.where(
                    low, pltpu.roll(first, LANES - shift, 1), second
                )
        pieces = following
        distance //= 2
    return pieces


def gram_kernel(moved_ref, basis_ref, out_ref, *, depths, offsets, row_low):
    lat_devices, tm_devices, _, _, groups, _ = moved_ref.shape
    total = None
    for slot, depth in enumerate(depths):
        pieces = [
            moved_ref[:, tm, slot, part].astype(jnp.float32).reshape(lat_devices * groups, LANES)
            for part in range(2)
            for tm in range(tm_devices)
        ]
        tiles = []
        for begin in range(0, len(pieces), row_low):
            tiles.append(exchange_blocks(pieces[begin : begin + row_low]))
        fourier = jnp.concatenate(
            [
                jnp.concatenate([tile[row] for tile in tiles], axis=1)
                for row in range(row_low)
            ],
            axis=0,
        ).astype(jnp.bfloat16)
        basis = basis_ref[offsets[slot] : offsets[slot] + depth, :]
        coefficients = jnp.dot(basis, fourier, preferred_element_type=jnp.float32)
        coefficients = coefficients.astype(jnp.bfloat16)
        gram = lax.dot_general(
            coefficients,
            coefficients,
            (((0,), (0,)), ((), ())),
            preferred_element_type=jnp.float32,
        )
        total = gram if total is None else total + gram
    months = total.shape[0] // 2
    total = total * (1.0 / (SCALE * SCALE))
    if len(out_ref.shape) == 2:
        out_ref[...] = total[:months, :months] + total[months:, months:]
        return
    half = months // 2
    quarter = half // 2
    lane = lax.broadcasted_iota(jnp.int32, (half, LANES), 1)
    row = lax.broadcasted_iota(jnp.int32, (half, LANES), 0)
    low = total[0:half] + pltpu.roll(total[months : months + half], months, 1)
    high = pltpu.roll(total[half:months], months, 1) + total[months + half :]
    packed = jnp.where(lane < months, low, high)
    trace = jnp.sum(jnp.where((lane == row) | (lane == row + months + half), packed, 0.0))
    lane = lane[:quarter]
    row = row[:quarter]
    swapped = pltpu.roll(packed, months, 1)
    halves = (
        jnp.where(lane < months, packed[:quarter], swapped[quarter:]),
        jnp.where(lane < months, swapped[:quarter], packed[quarter:]),
    )
    for index, value in enumerate(halves):
        value = jnp.where((row == 1) & (lane == index * half), trace, value)
        for device in range(index, out_ref.shape[0], 2):
            out_ref[device] = value


def gram_terms(moved, basis, depths, offsets, row_low, spread):
    months = moved.shape[1] * (LANES // row_low)
    shape = (spread, months // 4, LANES) if spread else (months, months)
    return pl.pallas_call(
        lambda *refs: gram_kernel(*refs, depths=depths, offsets=offsets, row_low=row_low),
        in_specs=[pl.BlockSpec(memory_space=pltpu.VMEM)] * 2,
        out_specs=pl.BlockSpec(memory_space=pltpu.VMEM),
        out_shape=pltpu.VMEM(shape, jnp.float32),
        compiler_params=PARAMS,
        name="gram",
    )(
        pltpu.with_memory_space_constraint(moved, pltpu.VMEM),
        pltpu.with_memory_space_constraint(basis, pltpu.VMEM),
    )


def finish_kernel(parts_ref, out_ref):
    half, month_total = out_ref.shape
    total = jnp.sum(parts_ref[...], axis=0)
    row = lax.broadcasted_iota(jnp.int32, total.shape, 0)
    lane = lax.broadcasted_iota(jnp.int32, total.shape, 1)
    corner = lane - lax.axis_index("tm") * half
    slot = (row == 1) & (corner == 0)
    trace = jnp.sum(jnp.where(slot, total, 0.0))
    mirror = jnp.sum(jnp.where((row == 0) & (corner == 1), total, 0.0))
    total = jnp.where(slot, mirror, total)
    total = month_total * total / (trace + 1e-06)
    out_ref[: half // 2] = total[:, :month_total]
    out_ref[half // 2 :] = pltpu.roll(total, month_total, 1)[:, :month_total]


def local(fields):
    row_count, month_count, lon_count = fields.shape
    lat_devices = lax.axis_size("lat")
    tm_devices = lax.axis_size("tm")
    device_total = lat_devices * tm_devices
    device = lax.axis_index("lat") * tm_devices + lax.axis_index("tm")
    lat_count = row_count * lat_devices
    months = month_count * tm_devices
    slots = -(-(TRUNC + 1) // device_total)
    row_low = LANES // month_count
    groups = row_count // row_low
    depths = [-(-(TRUNC + 1 - slot * device_total) // 16) * 16 for slot in range(slots)]
    offsets = [sum(depths[:slot]) for slot in range(slots)]

    table = jnp.asarray(transform_table(lon_count, device_total, slots))
    fourier = longitude_transform(fields, table, groups)
    fourier = fourier.reshape(device_total, slots * 2, groups, LANES)
    moved = lax.all_to_all(fourier, ("lat", "tm"), split_axis=0, concat_axis=0, tiled=True)
    moved = moved.reshape(lat_devices, tm_devices, slots, 2, groups, LANES)

    latitude = np.arange(lat_count).reshape(lat_devices, groups, row_low)
    latitude = jnp.asarray(latitude.transpose(2, 0, 1).reshape(1, -1))
    theta = math.pi * (latitude.astype(jnp.float32) + 0.5) / lat_count
    cosine_lat = jnp.cos(theta)
    sine_lat = jnp.sin(theta)
    weight = math.pi * sine_lat / lat_count
    padded = -(-slots // SUB) * SUB
    order = (jnp.arange(padded) * device_total + device).astype(jnp.float32)[:, None]
    log_start = 0.5 * (
        math.log(0.5)
        + lax.lgamma(order + 1.5)
        - (0.5 * math.log(math.pi) - math.log(2.0))
        - lax.lgamma(order + 1.0)
    ) + order * jnp.log(sine_lat)
    taper = jnp.clip((log_start + 70.0) / 10.0, 0.0, 1.0)
    factor = jnp.where(order > 0, math.sqrt(2.0), 1.0) * (order <= TRUNC) * SCALE
    start = jnp.exp(jnp.maximum(log_start, -80.0)) * taper * weight * factor
    basis = basis_blocks(
        jnp.broadcast_to(order, (padded, LANES)), cosine_lat, start, depths, offsets
    )

    spread = device_total if 2 * months == LANES and tm_devices == 2 else 0
    gram = gram_terms(moved, basis, depths, offsets, row_low, spread)
    if spread:
        parts = lax.all_to_all(gram, ("lat", "tm"), split_axis=0, concat_axis=0, tiled=True)
        return pl.pallas_call(
            finish_kernel,
            out_shape=jax.ShapeDtypeStruct((month_count, months), jnp.float32),
            compiler_params=PARAMS,
        name="finish",
        )(parts)
    gram = lax.psum(gram, ("lat", "tm"))
    trace = jnp.sum(jnp.diagonal(gram))
    own = lax.dynamic_slice_in_dim(gram, lax.axis_index("tm") * month_count, month_count, 0)
    return months * own / (trace + 1e-06)


def solution(mesh):
    placed = (P("lat", "tm", None),)
    return jax.shard_map(
        local, mesh=mesh, in_specs=placed, out_specs=P("tm", None), check_vma=False
    )
```

```python
import math

import numpy as np
import jax
import jax.numpy as jnp
from jax import lax
from jax.experimental import pallas as pl
from jax.experimental.pallas import tpu as pltpu
from jax.sharding import PartitionSpec as P

TRUNC = 341
LANES = 128
SUB = 8
STEPS = 32
SCALE = 2.0**16
PARAMS = pltpu.CompilerParams(vmem_limit_bytes=32 * 2**20)


def transform_table(lon_count, device_total, slot_total):
    order = np.arange(slot_total)[None, :] * device_total + np.arange(device_total)[:, None]
    order = order.reshape(-1, 1)
    phase = 2.0 * np.pi * (order * np.arange(lon_count)[None, :] % lon_count) / lon_count
    active = (order <= TRUNC) / np.sqrt(lon_count)
    table = np.stack([np.cos(phase) * active, -np.sin(phase) * active], axis=1)
    return table.reshape(-1, lon_count).astype(np.float32).astype(jnp.bfloat16)


def transform_kernel(table_ref, fields_ref, out_ref, scratch_ref):
    step = pl.program_id(0)
    groups = out_ref.shape[1]
    column_total, lon_count = table_ref.shape
    block = fields_ref[...].reshape(-1, lon_count)
    values = lax.dot_general(
        table_ref[...], block, (((1,), (1,)), ((), ())), preferred_element_type=jnp.float32
    )
    for part in range(values.shape[1] // LANES):
        group = step * (values.shape[1] // LANES) + part
        scratch_ref[pl.ds(group, column_total, stride=groups), :] = values[
            :, part * LANES : (part + 1) * LANES
        ]

    @pl.when(step == pl.num_programs(0) - 1)
    def _():
        out_ref[...] = scratch_ref[...].reshape(out_ref.shape).astype(out_ref.dtype)


def longitude_transform(fields, table, groups):
    row_count, month_count, lon_count = fields.shape
    column_total = table.shape[0]
    rows_step = 2 * LANES // month_count
    return pl.pallas_call(
        transform_kernel,
        grid=(row_count // rows_step,),
        in_specs=[
            pl.BlockSpec((column_total, lon_count), lambda g: (0, 0)),
            pl.BlockSpec((rows_step, month_count, lon_count), lambda g: (g, 0, 0)),
        ],
        out_specs=pl.BlockSpec((column_total, groups, LANES), lambda g: (0, 0, 0)),
        out_shape=jax.ShapeDtypeStruct((column_total, groups, LANES), jnp.bfloat16),
        scratch_shapes=[pltpu.VMEM((column_total * groups, LANES), jnp.float32)],
        compiler_params=PARAMS,
        name="transform",
    )(
        pltpu.with_memory_space_constraint(table, pltpu.HBM),
        pltpu.with_memory_space_constraint(fields, pltpu.HBM),
    )


def basis_kernel(order_ref, cosine_ref, start_ref, out_ref, scratch_ref, *, depths, offsets):
    cosine = jnp.broadcast_to(cosine_ref[...], (SUB, cosine_ref.shape[1]))
    for base in range(0, len(depths), SUB):
        order = order_ref[base : base + SUB, :]
        lane = lax.broadcasted_iota(jnp.int32, order.shape, 1).astype(jnp.float32)
        first = start_ref[base : base + SUB, :]
        columns = scratch_ref.shape[0]
        for column in range(columns):
            scratch_ref[column, 0:SUB, :] = first[:, column * LANES : (column + 1) * LANES]

        def block(index, carry, order=order, lane=lane, columns=columns):
            current, previous = carry
            degree = order + (lane + 1.0) + (index * STEPS).astype(jnp.float32)
            top = jnp.sqrt((4.0 * degree * degree - 1.0) / (degree * degree - order * order))
            below = degree - 1.0
            back = jnp.sqrt(
                jnp.maximum(below * below - order * order, 0.0)
                / jnp.abs(4.0 * below * below - 1.0)
            )
            inside = degree <= TRUNC
            mixed = jnp.where(inside, top * back, 0.0)
            top = jnp.where(inside, top, 0.0)
            for step in range(STEPS):
                top_step = top[:, step : step + 1] * cosine
                following = top_step * current - mixed[:, step : step + 1] * previous
                row = pl.multiple_of((index * STEPS + (step + 1)) * SUB, SUB)
                for column in range(columns):
                    scratch_ref[column, pl.ds(row, SUB), :] = following[
                        :, column * LANES : (column + 1) * LANES
                    ]
                current, previous = following, current
            return current, previous

        depth_most = depths[base]
        lax.fori_loop(0, pl.cdiv(depth_most - 1, STEPS), block, (first, jnp.zeros_like(first)))
        for slot in range(base, min(base + SUB, len(depths))):
            depth = depths[slot]
            for column in range(columns):
                rows = scratch_ref[column, pl.ds(slot - base, depth, stride=SUB), :]
                out_ref[
                    offsets[slot] : offsets[slot] + depth, column * LANES : (column + 1) * LANES
                ] = rows.astype(out_ref.dtype)


def basis_blocks(order, cosine, start, depths, offsets):
    lat_total = cosine.shape[1]
    steps_most = pl.cdiv(max(depths) - 1, STEPS) * STEPS + 1
    return pl.pallas_call(
        lambda *refs: basis_kernel(*refs, depths=depths, offsets=offsets),
        out_shape=pltpu.VMEM((sum(depths), lat_total), jnp.bfloat16),
        scratch_shapes=[pltpu.VMEM((lat_total // LANES, steps_most * SUB, LANES), jnp.float32)],
        out_specs=pl.BlockSpec(memory_space=pltpu.VMEM),
        compiler_params=PARAMS,
        name="basis",
    )(order, cosine, start)


def exchange_blocks(pieces):
    count = len(pieces)
    width = LANES // count
    block = lax.broadcasted_iota(jnp.int32, pieces[0].shape, 1) // width
    distance = count // 2
    while distance >= 1:
        low = (block // distance) % 2 == 0
        shift = distance * width
        following = list(pieces)
        for index in range(count):
            if (index // distance) % 2 == 0:
                first, second = pieces[index], pieces[index + distance]
                following[index] = jnp.where(low, first, pltpu.roll(second, shift, 1))
                following[index + distance] = jnp.where(
                    low, pltpu.roll(first, LANES - shift, 1), second
                )
        pieces = following
        distance //= 2
    return pieces


def gram_kernel(early_ref, late_ref, basis_ref, out_ref, *, depths, offsets, row_low):
    lat_devices, tm_devices, early, _, groups, _ = early_ref.shape
    total = None
    for slot, depth in enumerate(depths):
        moved_ref, place = (early_ref, slot) if slot < early else (late_ref, slot - early)
        pieces = [
            moved_ref[:, tm, place, part].astype(jnp.float32).reshape(lat_devices * groups, LANES)
            for part in range(2)
            for tm in range(tm_devices)
        ]
        tiles = []
        for begin in range(0, len(pieces), row_low):
            tiles.append(exchange_blocks(pieces[begin : begin + row_low]))
        fourier = jnp.concatenate(
            [
                jnp.concatenate([tile[row] for tile in tiles], axis=1)
                for row in range(row_low)
            ],
            axis=0,
        ).astype(jnp.bfloat16)
        basis = basis_ref[offsets[slot] : offsets[slot] + depth, :]
        coefficients = jnp.dot(basis, fourier, preferred_element_type=jnp.float32)
        coefficients = coefficients.astype(jnp.bfloat16)
        gram = lax.dot_general(
            coefficients,
            coefficients,
            (((0,), (0,)), ((), ())),
            preferred_element_type=jnp.float32,
        )
        total = gram if total is None else total + gram
    months = total.shape[0] // 2
    total = total * (1.0 / (SCALE * SCALE))
    if len(out_ref.shape) == 2:
        out_ref[...] = total[:months, :months] + total[months:, months:]
        return
    half = months // 2
    quarter = half // 2
    lane = lax.broadcasted_iota(jnp.int32, (half, LANES), 1)
    row = lax.broadcasted_iota(jnp.int32, (half, LANES), 0)
    low = total[0:half] + pltpu.roll(total[months : months + half], months, 1)
    high = pltpu.roll(total[half:months], months, 1) + total[months + half :]
    packed = jnp.where(lane < months, low, high)
    trace = jnp.sum(jnp.where((lane == row) | (lane == row + months + half), packed, 0.0))
    lane = lane[:quarter]
    row = row[:quarter]
    swapped = pltpu.roll(packed, months, 1)
    halves = (
        jnp.where(lane < months, packed[:quarter], swapped[quarter:]),
        jnp.where(lane < months, swapped[:quarter], packed[quarter:]),
    )
    for index, value in enumerate(halves):
        value = jnp.where((row == 1) & (lane == index * half), trace, value)
        for device in range(index, out_ref.shape[0], 2):
            out_ref[device] = value


def gram_terms(moved, basis, depths, offsets, row_low, spread):
    months = moved[0].shape[1] * (LANES // row_low)
    shape = (spread, months // 4, LANES) if spread else (months, months)
    return pl.pallas_call(
        lambda *refs: gram_kernel(*refs, depths=depths, offsets=offsets, row_low=row_low),
        in_specs=[pl.BlockSpec(memory_space=pltpu.VMEM)] * 3,
        out_specs=pl.BlockSpec(memory_space=pltpu.VMEM),
        out_shape=pltpu.VMEM(shape, jnp.float32),
        compiler_params=PARAMS,
        name="gram",
    )(
        *(pltpu.with_memory_space_constraint(part, pltpu.VMEM) for part in moved),
        pltpu.with_memory_space_constraint(basis, pltpu.VMEM),
    )


def finish_kernel(parts_ref, out_ref):
    half, month_total = out_ref.shape
    total = jnp.sum(parts_ref[...], axis=0)
    row = lax.broadcasted_iota(jnp.int32, total.shape, 0)
    lane = lax.broadcasted_iota(jnp.int32, total.shape, 1)
    corner = lane - lax.axis_index("tm") * half
    slot = (row == 1) & (corner == 0)
    trace = jnp.sum(jnp.where(slot, total, 0.0))
    mirror = jnp.sum(jnp.where((row == 0) & (corner == 1), total, 0.0))
    total = jnp.where(slot, mirror, total)
    total = month_total * total / (trace + 1e-06)
    out_ref[: half // 2] = total[:, :month_total]
    out_ref[half // 2 :] = pltpu.roll(total, month_total, 1)[:, :month_total]


def local(fields):
    row_count, month_count, lon_count = fields.shape
    lat_devices = lax.axis_size("lat")
    tm_devices = lax.axis_size("tm")
    device_total = lat_devices * tm_devices
    device = lax.axis_index("lat") * tm_devices + lax.axis_index("tm")
    lat_count = row_count * lat_devices
    months = month_count * tm_devices
    slots = -(-(TRUNC + 1) // device_total)
    row_low = LANES // month_count
    groups = row_count // row_low
    depths = [-(-(TRUNC + 1 - slot * device_total) // 16) * 16 for slot in range(slots)]
    offsets = [sum(depths[:slot]) for slot in range(slots)]

    table = transform_table(lon_count, device_total, slots)
    table = table.reshape(device_total, slots * 2, lon_count)
    moved = []
    split = slots // 2
    for begin, end in ((0, split), (split, slots)) if split else ((0, slots), (0, slots)):
        part = jnp.asarray(table[:, 2 * begin : 2 * end].reshape(-1, lon_count))
        fourier = longitude_transform(fields, part, groups)
        fourier = fourier.reshape(device_total, (end - begin) * 2, groups, LANES)
        part = lax.all_to_all(fourier, ("lat", "tm"), split_axis=0, concat_axis=0, tiled=True)
        moved.append(part.reshape(lat_devices, tm_devices, end - begin, 2, groups, LANES))

    latitude = np.arange(lat_count).reshape(lat_devices, groups, row_low)
    latitude = jnp.asarray(latitude.transpose(2, 0, 1).reshape(1, -1))
    theta = math.pi * (latitude.astype(jnp.float32) + 0.5) / lat_count
    cosine_lat = jnp.cos(theta)
    sine_lat = jnp.sin(theta)
    weight = math.pi * sine_lat / lat_count
    padded = -(-slots // SUB) * SUB
    order = (jnp.arange(padded) * device_total + device).astype(jnp.float32)[:, None]
    log_start = 0.5 * (
        math.log(0.5)
        + lax.lgamma(order + 1.5)
        - (0.5 * math.log(math.pi) - math.log(2.0))
        - lax.lgamma(order + 1.0)
    ) + order * jnp.log(sine_lat)
    taper = jnp.clip((log_start + 70.0) / 10.0, 0.0, 1.0)
    factor = jnp.where(order > 0, math.sqrt(2.0), 1.0) * (order <= TRUNC) * SCALE
    start = jnp.exp(jnp.maximum(log_start, -80.0)) * taper * weight * factor
    basis = basis_blocks(
        jnp.broadcast_to(order, (padded, LANES)), cosine_lat, start, depths, offsets
    )

    spread = device_total if 2 * months == LANES and tm_devices == 2 else 0
    gram = gram_terms(moved, basis, depths, offsets, row_low, spread)
    if spread:
        parts = lax.all_to_all(gram, ("lat", "tm"), split_axis=0, concat_axis=0, tiled=True)
        return pl.pallas_call(
            finish_kernel,
            out_shape=jax.ShapeDtypeStruct((month_count, months), jnp.float32),
            compiler_params=PARAMS,
        name="finish",
        )(parts)
    gram = lax.psum(gram, ("lat", "tm"))
    trace = jnp.sum(jnp.diagonal(gram))
    own = lax.dynamic_slice_in_dim(gram, lax.axis_index("tm") * month_count, month_count, 0)
    return months * own / (trace + 1e-06)


def solution(mesh):
    placed = (P("lat", "tm", None),)
    return jax.shard_map(
        local, mesh=mesh, in_specs=placed, out_specs=P("tm", None), check_vma=False
    )
```
